128 devices in a mesh: grp: 16 (over z, x), ep: 8 (over y, core).
Axes of the slice: x: 4, y: 4, z: 4, core: 2. Of those that a mesh axis runs over, the one named last changes fastest.
Arguments:
- tokens: bfloat16 [256, 7168], P(('grp', 'ep')), may hold values from -6 to 6
- expert_ids: int32 [256, 8], P(('grp', 'ep')), may hold values from 0 to 15, all different within a row; in each aligned block of 2 rows (0 to 1, 2 to 3, ...) at most 2 rows name the same one
- gate_ints: int32 [256, 8], P(('grp', 'ep')), may hold values from 1 to 16
- w_gate: bfloat16 [16, 7168, 2048], P('grp', None, 'ep'), may hold values from -0.0625 to 0.0625
- w_up: bfloat16 [16, 7168, 2048], P('grp', None, 'ep'), may hold values from -0.0625 to 0.0625
- w_down: bfloat16 [16, 2048, 7168], P('grp', 'ep'), may hold values from -0.125 to 0.125
Outputs:
- mixed: bfloat16 [256, 7168], P(('grp', 'ep'))
The draws below stay inside these ranges and needn't reach their ends.
Inputs may be any that keep to these rules, and one draw needn't show every extreme that they name: `expert_ids`: each row names 8 different experts. Within the 2 rows of one device no expert is named more than 2 times, a bound that some block reaches on some device in every draw.
All inputs are finite; a program needn't handle non-finite values.
Results may differ from the reference program's by a relative error of at most 0.015.
Values may be sent and summed in bfloat16 or wider, within the bound.
No kernel may reach another device: no remote copies, remote signals or barrier semaphores. Data moves between devices by JAX's collectives and lax.ppermute only.
A program may use at most 64 MiB of HBM per device.

```python
import math
import jax
import jax.numpy as jnp
import numpy as np
from jax import lax

D = 7168
FF = 2048
TOPK = 8
TOK_DEV = 2
EXPERTS = 16
CAP = 2
TOKENS = 256
DEVICES = 128


def place_ends(values, own_key, least, largest):
    shape = values.shape
    place = [jax.random.randint(jax.random.fold_in(own_key, axis), (), 0, shape[axis]) for axis in range(len(shape))]
    values = values.at[tuple(place)].set(least)
    longest = shape.index(max(shape))
    place[longest] = (place[longest] + 1) % shape[longest]
    return values.at[tuple(place)].set(largest)


def block_levels(rng, dims, cuts, low, top_value):
    factor_of, own = 1.0, jax.random.fold_in(rng, 6)
    for dim, shards_of in cuts:
        steps = jnp.exp(jax.random.uniform(jax.random.fold_in(own, dim), (shards_of,), jnp.float32, low / len(cuts), top_value / len(cuts)))
        factor_of = factor_of * jnp.repeat(steps, dims[dim] // shards_of).reshape([-1 if axis == dim else 1 for axis in range(len(dims))])
    return factor_of


def deal_out(stream_key, own, number, rows, number_of, top, reach, slope):
    sequence = jax.random.permutation(stream_key, number_of)
    heavy_load, common = shares(number_of, rows * top, reach, slope, True), shares(number_of, rows * top, reach, slope, False)
    places = jnp.arange(number_of)

    def named(tallies, turn):
        used = int((tallies > 0).sum())
        fixed = max(1, used // 4)
        moved = fixed + (places - fixed + turn * (used - fixed)) % max(1, number_of - fixed)
        return jnp.zeros((number_of,), jnp.int32).at[sequence[jnp.where(places < fixed, places, moved)]].set(jnp.asarray(tallies, jnp.int32))

    tallies = jnp.where(number % 4 == 0, named(heavy_load, number // 4), named(common, number - number // 4 - 1))
    mixed = jax.random.permutation(jax.random.fold_in(own, 3), number_of)
    giver, sink = mixed[0:number_of // 2 * 2:2], mixed[1:number_of // 2 * 2:2]
    margin = jnp.minimum(tallies[giver] - 1, reach - tallies[sink]) // 2
    margin = jnp.where((giver == sequence[0]) | (sink == sequence[0]) | (tallies[sink] == 0), 0, jnp.maximum(margin, 0))
    moved = jax.random.randint(jax.random.fold_in(own, 4), (number_of // 2,), 0, 1 << 20) % (margin + 1)
    tallies = tallies.at[giver].add(-moved).at[sink].add(moved)
    members = jnp.searchsorted(jnp.cumsum(tallies), jnp.arange(rows * top), side="right").astype(jnp.int32)
    grid = members.reshape(top, rows).T
    grid = grid[jax.random.permutation(jax.random.fold_in(own, 1), rows)]
    turn = jax.random.randint(jax.random.fold_in(own, 2), (rows, 1), 0, top)
    return jnp.take_along_axis(grid, (jnp.arange(top)[None, :] + turn) % top, axis=1)


def shares(count, total, limit, skew, full):
    portions = [(1 << 20) // math.isqrt(rank ** skew) + 1 for rank in range(1, count + 1)]
    largest = limit if full else min(limit, max(-(-total // count), total * portions[0] // sum(portions)))
    least = 1 if total - largest >= count - 1 else 0
    counts, spare = [largest] + [least] * (count - 1), total - largest - least * (count - 1)
    while spare > 0:
        candidates = [i for i in range(1, count) if counts[i] < largest] or [i for i in range(1, count) if counts[i] < limit]
        pool, budget = sum([portions[i] for i in candidates]), spare
        for i in candidates:
            addition = min(limit - counts[i], max(1, budget * portions[i] // pool), spare)
            counts[i] = counts[i] + addition
            spare = spare - addition
    return np.array(counts)


def bell_draw(rng, dims, scale, bound, pieces=(), kind=jnp.bfloat16):
    entries = scale * jax.random.normal(rng, dims, jnp.float32)
    if pieces:
        entries = entries * block_levels(rng, dims, pieces, -0.22, 0.18)
    return jnp.clip(entries, -bound, bound).astype(kind)


def setup_inputs(seed: int = 0) -> dict:
    key_of = jax.random.split(jax.random.key(seed), 7)
    tokens = bell_draw(key_of[0], (TOKENS, D), 1.0, 6.0, ((0, 128),))
    expert_ids_keys = jax.random.split(jax.random.fold_in(key_of[1], 1), TOKENS // TOK_DEV)
    expert_ids_turns = jax.random.permutation(jax.random.fold_in(key_of[1], 3), TOKENS // TOK_DEV)
    expert_ids = jax.vmap(lambda own, number: deal_out(jax.random.fold_in(key_of[1], 2), own, number, TOK_DEV, EXPERTS, TOPK, CAP, 1))(expert_ids_keys, expert_ids_turns).reshape((TOKENS, TOPK))
    gate_ints = place_ends(jax.random.randint(key_of[2], (TOKENS, TOPK), 1, 17), jax.random.fold_in(key_of[2], 1), 1, 16).astype(jnp.int32)
    w_gate = bell_draw(key_of[3], (EXPERTS, D, FF), D ** -0.5, 0.0625, ((0, 16), (2, 8)))
    w_up = bell_draw(key_of[4], (EXPERTS, D, FF), D ** -0.5, 0.0625, ((0, 16), (2, 8)))
    w_down = bell_draw(key_of[5], (EXPERTS, FF, D), FF ** -0.5, 0.125, ((0, 16), (1, 8)))
    return {"tokens": tokens, "expert_ids": expert_ids, "gate_ints": gate_ints, "w_gate": w_gate, "w_up": w_up, "w_down": w_down}


def slot_tables(expert_ids):
    routes = expert_ids.reshape(DEVICES, TOK_DEV * TOPK)
    onehot = (routes[:, :, None] == jnp.arange(EXPERTS, dtype=jnp.int32)[None, None, :]).astype(jnp.int32)
    earlier = jnp.cumsum(onehot, axis=1).astype(jnp.int32) - onehot
    slots = jnp.sum(earlier * onehot, axis=2).astype(jnp.int32)
    return routes, slots


def reference(tokens, expert_ids, gate_ints, w_gate, w_up, w_down):
    routes, slots = slot_tables(expert_ids)
    sources = jnp.arange(DEVICES, dtype=jnp.int32)[:, None]
    token_index = sources * TOK_DEV + jnp.arange(TOK_DEV * TOPK, dtype=jnp.int32)[None, :] // TOPK
    position = (routes * (DEVICES * CAP) + sources * CAP + slots).astype(jnp.int32).reshape(-1)
    table = jnp.zeros((EXPERTS * DEVICES * CAP,), jnp.int32).at[position].set(token_index.reshape(-1).astype(jnp.int32))
    filled = jnp.zeros((EXPERTS * DEVICES * CAP,), jnp.int32).at[position].set(1)
    table = table.reshape(EXPERTS, DEVICES * CAP)
    filled = filled.reshape(EXPERTS, DEVICES * CAP)

    def run_expert(operands):
        row_index, live, gate_w, up_w, down_w = operands
        rows = tokens[row_index] * live.astype(jnp.bfloat16)[:, None]
        gate = jnp.dot(rows, gate_w, preferred_element_type=jnp.float32)
        up = jnp.dot(rows, up_w, preferred_element_type=jnp.float32)
        hidden = (jax.nn.silu(gate) * up).astype(jnp.bfloat16)
        return jnp.dot(hidden, down_w, preferred_element_type=jnp.float32).astype(jnp.bfloat16)

    expert_out = lax.map(run_expert, (table, filled, w_gate, w_up, w_down))
    flat_out = expert_out.reshape(EXPERTS * DEVICES * CAP, D)
    scores = gate_ints.astype(jnp.float32)
    weight = scores / jnp.sum(scores, axis=1, keepdims=True)
    route_rows = position.reshape(TOKENS, TOPK)
    mixed = jnp.zeros((TOKENS, D), jnp.float32)
    for rank in range(TOPK):
        mixed = mixed + weight[:, rank:rank + 1] * flat_out[route_rows[:, rank]].astype(jnp.float32)
    return mixed.astype(jnp.bfloat16)
```

```python
import itertools

import jax
import jax.numpy as jnp
from jax import lax
from jax.experimental import pallas as pl
from jax.experimental.pallas import tpu as pltpu
from jax.sharding import Mesh
from jax.sharding import PartitionSpec as P

ALL = ("z", "x", "y", "c")
RING = 4
LANES = 128
KCH = 1024


def index(z, x, y, c):
    return ((z * RING + x) * RING + y) * 2 + c


def class_groups():
    groups = []
    for colour in range(RING):
        for c in range(2):
            members = []
            for z, y in itertools.product(range(RING), repeat=2):
                members.append(index(z, (colour + 2 * y + z) % RING, y, c))
            groups.append(members)
    return groups


def neighbour_pairs(axis, back):
    pairs = []
    for z, x, y in itertools.product(range(RING), repeat=3):
        for c in range(2):
            there = {"z": z, "x": x, "y": y}
            there[axis] = (there[axis] + (1 if c == 0 else -1)) % RING
            pair = (index(z, x, y, c), index(there["z"], there["x"], there["y"], c))
            pairs.append(pair[::-1] if back else pair)
    return pairs


def swap_pairs():
    return [(i, i ^ 1) for i in range(2 * RING**3)]


def experts_kernel(me_ref, b0, b1, b2, b3, other, wg_hbm, wu_hbm, wd_hbm, mine_ref, theirs_ref, wg, wu, wd, hid, sems):
    width = wg.shape[0]
    chunks = width // KCH
    copies = []
    for i in range(chunks):
        ks = pl.ds(i * KCH, KCH)
        pair = [
            pltpu.make_async_copy(wg_hbm.at[ks, :], wg.at[ks, :], sems.at[0, i]),
            pltpu.make_async_copy(wu_hbm.at[ks, :], wu.at[ks, :], sems.at[1, i]),
        ]
        for copy in pair:
            copy.start()
        copies.append(pair)
    down = []
    for i in range(chunks):
        ks = pl.ds(i * KCH, KCH)
        copy = pltpu.make_async_copy(wd_hbm.at[:, ks], wd.at[:, ks], sems.at[2, i])
        copy.start()
        down.append(copy)

    def rows(ks):
        return jnp.concatenate([r[:, ks] for r in (b0, b1, b2, b3, other)], axis=0)

    scores = rows(pl.ds(width, LANES)).astype(jnp.float32)
    lane = lax.broadcasted_iota(jnp.int32, scores.shape, 1)
    picked = jnp.sum(jnp.where(lane == me_ref[0], scores, 0.0), axis=1, keepdims=True)
    weight = picked / jnp.sum(scores, axis=1, keepdims=True)
    gate = up = None
    for i in range(chunks):
        ks = pl.ds(i * KCH, KCH)
        for copy in copies[i]:
            copy.wait()
        part = rows(ks)
        g = jnp.dot(part, wg[ks, :], preferred_element_type=jnp.float32)
        u = jnp.dot(part, wu[ks, :], preferred_element_type=jnp.float32)
        gate, up = (g, u) if gate is None else (gate + g, up + u)
    hid[...] = (gate / (1.0 + jnp.exp(-gate)) * up).astype(jnp.bfloat16)
    half = mine_ref.shape[0]
    for i in range(chunks):
        ks = pl.ds(i * KCH, KCH)
        down[i].wait()
        out = jnp.dot(hid[...], wd[:, ks], preferred_element_type=jnp.float32) * weight
        mine_ref[:, ks] = out[:half]
        theirs_ref[:, ks] = out[half:].astype(jnp.bfloat16)


def run_experts(me, blocks, other, wg, wu, wd):
    width, hidden = wg.shape
    rows = 2 * other.shape[0]
    half = rows // 2
    chunks = width // KCH
    vmem = pl.BlockSpec(memory_space=pltpu.VMEM)
    hbm = pl.BlockSpec(memory_space=pl.ANY)
    return pl.pallas_call(
        experts_kernel,
        out_shape=(
            jax.ShapeDtypeStruct((half, width), jnp.float32),
            jax.ShapeDtypeStruct((half, width), jnp.bfloat16),
        ),
        in_specs=[pl.BlockSpec(memory_space=pltpu.SMEM)] + [vmem] * 5 + [hbm] * 3,
        out_specs=(vmem, vmem),
        scratch_shapes=[
            pltpu.VMEM((width, hidden), jnp.bfloat16),
            pltpu.VMEM((width, hidden), jnp.bfloat16),
            pltpu.VMEM((hidden, width), jnp.bfloat16),
            pltpu.VMEM((rows, hidden), jnp.bfloat16),
            pltpu.SemaphoreType.DMA((3, chunks)),
        ],
        compiler_params=pltpu.CompilerParams(vmem_limit_bytes=48 * 1024 * 1024),
        name="experts",
    )(me, *blocks, other, wg, wu, wd)


def local(tokens, expert_ids, gate_ints, w_gate, w_up, w_down):
    width = tokens.shape[1]
    me = (lax.axis_index("z") * RING + lax.axis_index("x")).astype(jnp.int32).reshape(1)
    lane = jnp.arange(LANES, dtype=jnp.int32)
    named = expert_ids[:, :, None] == lane[None, None, :]
    scores = jnp.sum(jnp.where(named, gate_ints[:, :, None], 0), axis=1).astype(jnp.bfloat16)
    row = jnp.concatenate([tokens, scores], axis=1)
    groups = class_groups()
    n = len(groups[0])
    tiled = jnp.broadcast_to(row[None], (n, *row.shape))
    own = lax.all_to_all(tiled, ALL, split_axis=0, concat_axis=0, axis_index_groups=groups, tiled=True)
    own = own.reshape(n * row.shape[0], row.shape[1])
    blocks = [own] + [lax.ppermute(own, ALL, neighbour_pairs(a, False)) for a in "xyz"]
    other = lax.ppermute(jnp.concatenate(blocks, axis=0), ALL, swap_pairs())
    mine, theirs = run_experts(me, blocks, other, w_gate[0], w_up[0], w_down[0])
    back = lax.ppermute(theirs, ALL, swap_pairs())
    total = mine + back.astype(jnp.float32)
    size = own.shape[0]
    parts = [total[i * size:(i + 1) * size] for i in range(4)]
    acc = parts[0]
    for a, part in zip("xyz", parts[1:]):
        acc = acc + lax.ppermute(part.astype(jnp.bfloat16), ALL, neighbour_pairs(a, True)).astype(jnp.float32)
    pieces = acc.astype(jnp.bfloat16).reshape(n, tokens.shape[0], width)
    got = lax.all_to_all(pieces, ALL, split_axis=0, concat_axis=0, axis_index_groups=groups, tiled=True)
    return jnp.sum(got.astype(jnp.float32), axis=0).astype(jnp.bfloat16)


def solution(mesh):
    fine = Mesh(mesh.devices.reshape(RING, RING, RING, 2), ALL)
    in_specs = (
        P(ALL, None),
        P(ALL, None),
        P(ALL, None),
        P(("z", "x"), None, ("y", "c")),
        P(("z", "x"), None, ("y", "c")),
        P(("z", "x"), ("y", "c"), None),
    )
    return jax.shard_map(local, mesh=fine, in_specs=in_specs, out_specs=P(ALL, None), check_vma=False)
```

```python
import itertools

import jax
import jax.numpy as jnp
from jax import lax
from jax.experimental import pallas as pl
from jax.experimental.pallas import tpu as pltpu
from jax.sharding import Mesh
from jax.sharding import PartitionSpec as P

ALL = ("z", "x", "y", "c")
RING = 4
LANES = 128
KCH = 1024
RATE = 250


def index(z, x, y, c):
    return ((z * RING + x) * RING + y) * 2 + c


def class_groups():
    groups = []
    for colour in range(RING):
        for c in range(2):
            members = []
            for z, y in itertools.product(range(RING), repeat=2):
                members.append(index(z, (colour + 2 * y + z) % RING, y, c))
            groups.append(members)
    return groups


def neighbour_pairs(axis, back):
    pairs = []
    for z, x, y in itertools.product(range(RING), repeat=3):
        for c in range(2):
            there = {"z": z, "x": x, "y": y}
            there[axis] = (there[axis] + (1 if c == 0 else -1)) % RING
            pair = (index(z, x, y, c), index(there["z"], there["x"], there["y"], c))
            pairs.append(pair[::-1] if back else pair)
    return pairs


def swap_pairs():
    return [(i, i ^ 1) for i in range(2 * RING**3)]


def head_kernel(me_ref, tok_hbm, ids_hbm, ints_hbm, out_ref, tok, ids_ref, ints_ref, sems):
    width = tok.shape[1]
    copies = [
        pltpu.make_async_copy(src, dst, sems.at[i])
        for i, (src, dst) in enumerate(((ids_hbm, ids_ref), (ints_hbm, ints_ref), (tok_hbm, tok)))
    ]
    for copy in copies:
        copy.start()
    for copy in copies:
        copy.wait()
    ids, ints = ids_ref[...], ints_ref[...]
    lane = lax.broadcasted_iota(jnp.int32, (ids.shape[0], LANES), 1)
    scores = jnp.zeros(lane.shape, jnp.float32)
    for k in range(ids.shape[1]):
        scores += jnp.where(ids[:, k:k + 1] == lane, ints[:, k:k + 1], 0).astype(jnp.float32)
    scores = scores.astype(jnp.bfloat16)
    token = tok[...]
    for i in range(out_ref.shape[0]):
        out_ref[i, :, :width] = token
        out_ref[i, :, width:] = scores


def load_kernel(wg_hbm, wu_hbm, wd_hbm, after_ref, wg, wu, wd, sems):
    copies = [
        pltpu.make_async_copy(src, dst, sems.at[i])
        for i, (src, dst) in enumerate(((wg_hbm, wg), (wu_hbm, wu), (wd_hbm, wd)))
    ]
    for copy in copies:
        copy.start()
    for copy in copies:
        copy.wait()


def experts_kernel(me_ref, mine_in, theirs_in, wg, wu, wd, after_ref, mine_out, theirs_out, hid):
    width = wg.shape[0]
    size = mine_in.shape[0]

    def rows(ks):
        return jnp.concatenate([mine_in[:, ks], theirs_in[:, ks]], axis=0)

    scores = rows(pl.ds(width, LANES)).astype(jnp.float32)
    lane = lax.broadcasted_iota(jnp.int32, scores.shape, 1)
    picked = jnp.sum(jnp.where(lane == me_ref[0], scores, 0.0), axis=1, keepdims=True)
    weight = picked / jnp.sum(scores, axis=1, keepdims=True)
    gate = up = None
    for i in range(width // KCH):
        ks = pl.ds(i * KCH, KCH)
        part = rows(ks)
        g = jnp.dot(part, wg[ks, :], preferred_element_type=jnp.float32)
        u = jnp.dot(part, wu[ks, :], preferred_element_type=jnp.float32)
        gate, up = (g, u) if gate is None else (gate + g, up + u)
    hid[...] = (gate / (1.0 + jnp.exp(-gate)) * up).astype(jnp.bfloat16)
    for i in range(width // KCH):
        ks = pl.ds(i * KCH, KCH)
        out = jnp.dot(hid[...], wd[:, ks], preferred_element_type=jnp.float32) * weight
        mine_out[:, ks] = out[:size]
        theirs_out[:, ks] = out[size:].astype(jnp.bfloat16)


def run_experts(me, mine, theirs, weights, after):
    size = mine.shape[0]
    width, hidden = weights[0].shape
    return pl.pallas_call(
        experts_kernel,
        out_shape=(
            jax.ShapeDtypeStruct((size, width), jnp.float32),
            jax.ShapeDtypeStruct((size, width), jnp.bfloat16),
        ),
        in_specs=[SMEM] + [VMEM] * 5 + [pl.BlockSpec(memory_space=pl.ANY)],
        out_specs=(VMEM, VMEM),
        scratch_shapes=[pltpu.VMEM((2 * size, hidden), jnp.bfloat16)],
        compiler_params=LIMIT,
        cost_estimate=cost(1.0),
    )(me, mine, theirs, *weights, after)


VMEM = pl.BlockSpec(memory_space=pltpu.VMEM)
SMEM = pl.BlockSpec(memory_space=pltpu.SMEM)
HBM = pl.BlockSpec(memory_space=pltpu.HBM)
LIMIT = pltpu.CompilerParams(vmem_limit_bytes=24 * 1024 * 1024)


def cost(us):
    return pl.CostEstimate(flops=int(us * 1e6 * RATE), transcendentals=0, bytes_accessed=0)


def in_hbm(*arrays):
    return [pltpu.with_memory_space_constraint(a, pltpu.HBM) for a in arrays]


def moved(block, pairs):
    return lax.ppermute(block, ALL, pairs)


def step(tokens, expert_ids, gate_ints, w_gate, w_up, w_down):
    width = tokens.shape[1]
    me = (lax.axis_index("z") * RING + lax.axis_index("x")).astype(jnp.int32).reshape(1)
    groups = class_groups()
    n = len(groups[0])
    bf16, f32 = jnp.bfloat16, jnp.float32

    tiled = pl.pallas_call(
        head_kernel,
        out_shape=jax.ShapeDtypeStruct((n, tokens.shape[0], width + LANES), bf16),
        in_specs=[SMEM] + [HBM] * 3,
        out_specs=VMEM,
        scratch_shapes=[
            pltpu.VMEM(tokens.shape, bf16),
            pltpu.VMEM(expert_ids.shape, jnp.int32),
            pltpu.VMEM(gate_ints.shape, jnp.int32),
            pltpu.SemaphoreType.DMA((3,)),
        ],
        compiler_params=LIMIT,
        name="head",
    )(me, *in_hbm(tokens, expert_ids, gate_ints))
    own = lax.all_to_all(tiled, ALL, split_axis=0, concat_axis=0, axis_index_groups=groups, tiled=True)
    own = own.reshape(n * tokens.shape[0], width + LANES)
    wg, wu, wd = pl.pallas_call(
        load_kernel,
        out_shape=[jax.ShapeDtypeStruct(w.shape[1:], bf16) for w in (w_gate, w_up, w_down)],
        in_specs=[HBM] * 3 + [pl.BlockSpec(memory_space=pl.ANY)],
        out_specs=[VMEM] * 3,
        scratch_shapes=[pltpu.SemaphoreType.DMA((3,))],
        compiler_params=LIMIT,
        cost_estimate=cost(3.4),
        name="load",
    )(*in_hbm(w_gate[0], w_up[0], w_down[0]), own)

    near = {a: moved(own, neighbour_pairs(a, False)) for a in "xyz"}
    near["o"] = own
    swapped = {a: moved(b, swap_pairs()) for a, b in near.items()}
    total = {}
    after = me
    for a in "oxyz":
        mine, theirs = run_experts(me, near[a], swapped[a], (wg, wu, wd), after)
        after = theirs
        total[a] = mine + moved(theirs, swap_pairs()).astype(f32)
    acc = total["o"]
    for a in "xyz":
        acc = acc + moved(total[a].astype(bf16), neighbour_pairs(a, True)).astype(f32)
    pieces = acc.astype(bf16).reshape(n, tokens.shape[0], width)
    got = lax.all_to_all(pieces, ALL, split_axis=0, concat_axis=0, axis_index_groups=groups, tiled=True)
    return jnp.sum(got.astype(f32), axis=0).astype(bf16)


def solution(mesh):
    fine = Mesh(mesh.devices.reshape(RING, RING, RING, 2), ALL)
    in_specs = (
        P(ALL, None),
        P(ALL, None),
        P(ALL, None),
        P(("z", "x"), None, ("y", "c")),
        P(("z", "x"), None, ("y", "c")),
        P(("z", "x"), ("y", "c"), None),
    )
    return jax.shard_map(step, mesh=fine, in_specs=in_specs, out_specs=P(ALL, None), check_vma=False)
```

```python
import itertools

import jax
import jax.numpy as jnp
from jax import lax
from jax.experimental import pallas as pl
from jax.experimental.pallas import tpu as pltpu
from jax.sharding import Mesh
from jax.sharding import PartitionSpec as P

ALL = ("z", "x", "y", "c")
RING = 4
LANES = 128
KCH = 1024
RATE = 250


def index(z, x, y, c):
    return ((z * RING + x) * RING + y) * 2 + c


def class_groups():
    groups = []
    for colour in range(RING):
        for c in range(2):
            members = []
            for z, y in itertools.product(range(RING), repeat=2):
                members.append(index(z, (colour + 2 * y + z) % RING, y, c))
            groups.append(members)
    return groups


def neighbour_pairs(axis, back):
    pairs = []
    for z, x, y in itertools.product(range(RING), repeat=3):
        for c in range(2):
            there = {"z": z, "x": x, "y": y}
            there[axis] = (there[axis] + (1 if c == 0 else -1)) % RING
            pair = (index(z, x, y, c), index(there["z"], there["x"], there["y"], c))
            pairs.append(pair[::-1] if back else pair)
    return pairs


def swap_pairs():
    return [(i, i ^ 1) for i in range(2 * RING**3)]


def head_kernel(me_ref, tok_hbm, ids_hbm, ints_hbm, out_ref, tok, ids_ref, ints_ref, sems):
    width = tok.shape[1]
    copies = [
        pltpu.make_async_copy(src, dst, sems.at[i])
        for i, (src, dst) in enumerate(((ids_hbm, ids_ref), (ints_hbm, ints_ref), (tok_hbm, tok)))
    ]
    for copy in copies:
        copy.start()
    for copy in copies:
        copy.wait()
    ids, ints = ids_ref[...], ints_ref[...]
    lane = lax.broadcasted_iota(jnp.int32, (ids.shape[0], LANES), 1)
    scores = jnp.zeros(lane.shape, jnp.float32)
    for k in range(ids.shape[1]):
        scores += jnp.where(ids[:, k:k + 1] == lane, ints[:, k:k + 1], 0).astype(jnp.float32)
    scores = scores.astype(jnp.bfloat16)
    token = tok[...]
    for i in range(out_ref.shape[0]):
        out_ref[i, :, :width] = token
        out_ref[i, :, width:] = scores


def load_kernel(wg_hbm, wu_hbm, wd_hbm, after_ref, wg, wu, wd, sems):
    copies = [
        pltpu.make_async_copy(src, dst, sems.at[i])
        for i, (src, dst) in enumerate(((wg_hbm, wg), (wu_hbm, wu), (wd_hbm, wd)))
    ]
    for copy in copies:
        copy.start()
    for copy in copies:
        copy.wait()


def experts_kernel(me_ref, *refs):
    ins, (wg, wu, wd, after_ref), outs, hid = refs[:4], refs[4:8], refs[8:12], refs[12]
    width = wg.shape[0]
    size = ins[0].shape[0]

    def rows(ks):
        return jnp.concatenate([r[:, ks] for r in ins], axis=0)

    scores = rows(pl.ds(width, LANES)).astype(jnp.float32)
    lane = lax.broadcasted_iota(jnp.int32, scores.shape, 1)
    picked = jnp.sum(jnp.where(lane == me_ref[0], scores, 0.0), axis=1, keepdims=True)
    weight = picked / jnp.sum(scores, axis=1, keepdims=True)
    gate = up = None
    for i in range(width // KCH):
        ks = pl.ds(i * KCH, KCH)
        part = rows(ks)
        g = jnp.dot(part, wg[ks, :], preferred_element_type=jnp.float32)
        u = jnp.dot(part, wu[ks, :], preferred_element_type=jnp.float32)
        gate, up = (g, u) if gate is None else (gate + g, up + u)
    hid[...] = (gate / (1.0 + jnp.exp(-gate)) * up).astype(jnp.bfloat16)
    for i in range(width // KCH):
        ks = pl.ds(i * KCH, KCH)
        out = jnp.dot(hid[...], wd[:, ks], preferred_element_type=jnp.float32) * weight
        for j, ref in enumerate(outs):
            ref[:, ks] = out[j * size:(j + 1) * size].astype(ref.dtype)


def run_experts(me, mine, theirs, weights, after):
    size = mine[0].shape[0]
    width, hidden = weights[0].shape
    kinds = [jnp.float32] * 2 + [jnp.bfloat16] * 2
    outs = pl.pallas_call(
        experts_kernel,
        out_shape=[jax.ShapeDtypeStruct((size, width), kind) for kind in kinds],
        in_specs=[SMEM] + [VMEM] * 7 + [pl.BlockSpec(memory_space=pl.ANY)],
        out_specs=[VMEM] * 4,
        scratch_shapes=[pltpu.VMEM((4 * size, hidden), jnp.bfloat16)],
        compiler_params=LIMIT,
        cost_estimate=cost(1.8),
    )(me, *mine, *theirs, *weights, after)
    return outs[:2], outs[2:]


VMEM = pl.BlockSpec(memory_space=pltpu.VMEM)
SMEM = pl.BlockSpec(memory_space=pltpu.SMEM)
HBM = pl.BlockSpec(memory_space=pltpu.HBM)
LIMIT = pltpu.CompilerParams(vmem_limit_bytes=24 * 1024 * 1024)


def cost(us):
    return pl.CostEstimate(flops=int(us * 1e6 * RATE), transcendentals=0, bytes_accessed=0)


def in_hbm(*arrays):
    return [pltpu.with_memory_space_constraint(a, pltpu.HBM) for a in arrays]


def moved(block, pairs):
    return lax.ppermute(block, ALL, pairs)


def step(tokens, expert_ids, gate_ints, w_gate, w_up, w_down):
    width = tokens.shape[1]
    me = (lax.axis_index("z") * RING + lax.axis_index("x")).astype(jnp.int32).reshape(1)
    groups = class_groups()
    n = len(groups[0])
    bf16, f32 = jnp.bfloat16, jnp.float32

    tiled = pl.pallas_call(
        head_kernel,
        out_shape=jax.ShapeDtypeStruct((n, tokens.shape[0], width + LANES), bf16),
        in_specs=[SMEM] + [HBM] * 3,
        out_specs=VMEM,
        scratch_shapes=[
            pltpu.VMEM(tokens.shape, bf16),
            pltpu.VMEM(expert_ids.shape, jnp.int32),
            pltpu.VMEM(gate_ints.shape, jnp.int32),
            pltpu.SemaphoreType.DMA((3,)),
        ],
        compiler_params=LIMIT,
        name="head",
    )(me, *in_hbm(tokens, expert_ids, gate_ints))
    own = lax.all_to_all(tiled, ALL, split_axis=0, concat_axis=0, axis_index_groups=groups, tiled=True)
    own = own.reshape(n * tokens.shape[0], width + LANES)
    wg, wu, wd = pl.pallas_call(
        load_kernel,
        out_shape=[jax.ShapeDtypeStruct(w.shape[1:], bf16) for w in (w_gate, w_up, w_down)],
        in_specs=[HBM] * 3 + [pl.BlockSpec(memory_space=pl.ANY)],
        out_specs=[VMEM] * 3,
        scratch_shapes=[pltpu.SemaphoreType.DMA((3,))],
        compiler_params=LIMIT,
        cost_estimate=cost(3.4),
        name="load",
    )(*in_hbm(w_gate[0], w_up[0], w_down[0]), own)

    near = {a: moved(own, neighbour_pairs(a, False)) for a in "xyz"}
    near["o"] = own
    swapped = {a: moved(b, swap_pairs()) for a, b in near.items()}
    total = {}
    after = me
    for pair in ("xo", "yz"):
        mine, theirs = run_experts(me, [near[a] for a in pair], [swapped[a] for a in pair], (wg, wu, wd), after)
        after = theirs[0]
        for a, kept, sent in zip(pair, mine, theirs):
            total[a] = kept + moved(sent, swap_pairs()).astype(f32)
    acc = total["o"]
    for a in "xyz":
        acc = acc + moved(total[a].astype(bf16), neighbour_pairs(a, True)).astype(f32)
    pieces = acc.astype(bf16).reshape(n, tokens.shape[0], width)
    got = lax.all_to_all(pieces, ALL, split_axis=0, concat_axis=0, axis_index_groups=groups, tiled=True)
    return jnp.sum(got.astype(f32), axis=0).astype(bf16)


def solution(mesh):
    fine = Mesh(mesh.devices.reshape(RING, RING, RING, 2), ALL)
    in_specs = (
        P(ALL, None),
        P(ALL, None),
        P(ALL, None),
        P(("z", "x"), None, ("y", "c")),
        P(("z", "x"), None, ("y", "c")),
        P(("z", "x"), ("y", "c"), None),
    )
    return jax.shard_map(step, mesh=fine, in_specs=in_specs, out_specs=P(ALL, None), check_vma=False)
```

```python
import itertools

import jax
import jax.numpy as jnp
from jax import lax
from jax.experimental import pallas as pl
from jax.experimental.pallas import tpu as pltpu
from jax.sharding import Mesh
from jax.sharding import PartitionSpec as P

ALL = ("z", "x", "y", "c")
RING = 4
LANES = 128
KCH = 1024
RATE = 250


def index(z, x, y, c):
    return ((z * RING + x) * RING + y) * 2 + c


def class_groups():
    groups = []
    for a, b, c in itertools.product(range(2), repeat=3):
        members = []
        for z, x, y in itertools.product(range(RING), repeat=3):
            if (x + z) % 2 == a and (y + z) % 2 == b:
                members.append(index(z, x, y, c))
        groups.append(members)
    return groups


def neighbour_pairs(axis):
    pairs = []
    for z, x, y in itertools.product(range(RING), repeat=3):
        for c in range(2):
            there = {"z": z, "x": x, "y": y}
            there[axis] = RING - 1 - there[axis] if c else there[axis] ^ 1
            pairs.append((index(z, x, y, c), index(there["z"], there["x"], there["y"], c)))
    return pairs


def swap_pairs():
    return [(i, i ^ 1) for i in range(2 * RING**3)]


def head_kernel(me_ref, tok_hbm, ids_hbm, ints_hbm, out_ref, tok, ids_ref, ints_ref, sems):
    width = tok.shape[1]
    copies = [
        pltpu.make_async_copy(src, dst, sems.at[i])
        for i, (src, dst) in enumerate(((ids_hbm, ids_ref), (ints_hbm, ints_ref), (tok_hbm, tok)))
    ]
    for copy in copies:
        copy.start()
    for copy in copies:
        copy.wait()
    ids, ints = ids_ref[...], ints_ref[...]
    lane = lax.broadcasted_iota(jnp.int32, (ids.shape[0], LANES), 1)
    scores = jnp.zeros(lane.shape, jnp.float32)
    for k in range(ids.shape[1]):
        scores += jnp.where(ids[:, k:k + 1] == lane, ints[:, k:k + 1], 0).astype(jnp.float32)
    scores = scores.astype(jnp.bfloat16)
    token = tok[...]
    for i in range(out_ref.shape[0]):
        out_ref[i, :, :width] = token
        out_ref[i, :, width:] = scores


def load_kernel(wg_hbm, wu_hbm, wd_hbm, after_ref, wg, wu, wd, sems):
    copies = [
        pltpu.make_async_copy(src, dst, sems.at[i])
        for i, (src, dst) in enumerate(((wg_hbm, wg), (wu_hbm, wu), (wd_hbm, wd)))
    ]
    for copy in copies:
        copy.start()
    for copy in copies:
        copy.wait()


def experts_kernel(me_ref, *refs):
    ins, (wg, wu, wd, after_ref), outs, hid = refs[:4], refs[4:8], refs[8:12], refs[12]
    width = wg.shape[0]
    size = ins[0].shape[0]

    def rows(ks):
        return jnp.concatenate([r[:, ks] for r in ins], axis=0)

    scores = rows(pl.ds(width, LANES)).astype(jnp.float32)
    lane = lax.broadcasted_iota(jnp.int32, scores.shape, 1)
    picked = jnp.sum(jnp.where(lane == me_ref[0], scores, 0.0), axis=1, keepdims=True)
    weight = picked / jnp.sum(scores, axis=1, keepdims=True)
    gate = up = None
    for i in range(width // KCH):
        ks = pl.ds(i * KCH, KCH)
        part = rows(ks)
        g = jnp.dot(part, wg[ks, :], preferred_element_type=jnp.float32)
        u = jnp.dot(part, wu[ks, :], preferred_element_type=jnp.float32)
        gate, up = (g, u) if gate is None else (gate + g, up + u)
    hid[...] = (gate / (1.0 + jnp.exp(-gate)) * up).astype(jnp.bfloat16)
    for i in range(width // KCH):
        ks = pl.ds(i * KCH, KCH)
        out = jnp.dot(hid[...], wd[:, ks], preferred_element_type=jnp.float32) * weight
        for j, ref in enumerate(outs):
            ref[:, ks] = out[j * size:(j + 1) * size].astype(ref.dtype)


def run_experts(me, mine, theirs, weights, after):
    size = mine[0].shape[0]
    width, hidden = weights[0].shape
    kinds = [jnp.float32] * 2 + [jnp.bfloat16] * 2
    outs = pl.pallas_call(
        experts_kernel,
        out_shape=[jax.ShapeDtypeStruct((size, width), kind) for kind in kinds],
        in_specs=[SMEM] + [VMEM] * 7 + [pl.BlockSpec(memory_space=pl.ANY)],
        out_specs=[VMEM] * 4,
        scratch_shapes=[pltpu.VMEM((4 * size, hidden), jnp.bfloat16)],
        compiler_params=LIMIT,
        cost_estimate=cost(1.8),
    )(me, *mine, *theirs, *weights, after)
    return outs[:2], outs[2:]


VMEM = pl.BlockSpec(memory_space=pltpu.VMEM)
SMEM = pl.BlockSpec(memory_space=pltpu.SMEM)
HBM = pl.BlockSpec(memory_space=pltpu.HBM)
LIMIT = pltpu.CompilerParams(vmem_limit_bytes=24 * 1024 * 1024)


def cost(us):
    return pl.CostEstimate(flops=int(us * 1e6 * RATE), transcendentals=0, bytes_accessed=0)


def in_hbm(*arrays):
    return [pltpu.with_memory_space_constraint(a, pltpu.HBM) for a in arrays]


def moved(block, pairs):
    return lax.ppermute(block, ALL, pairs)


def step(tokens, expert_ids, gate_ints, w_gate, w_up, w_down):
    width = tokens.shape[1]
    me = (lax.axis_index("z") * RING + lax.axis_index("x")).astype(jnp.int32).reshape(1)
    groups = class_groups()
    n = len(groups[0])
    bf16, f32 = jnp.bfloat16, jnp.float32

    tiled = pl.pallas_call(
        head_kernel,
        out_shape=jax.ShapeDtypeStruct((n, tokens.shape[0], width + LANES), bf16),
        in_specs=[SMEM] + [HBM] * 3,
        out_specs=VMEM,
        scratch_shapes=[
            pltpu.VMEM(tokens.shape, bf16),
            pltpu.VMEM(expert_ids.shape, jnp.int32),
            pltpu.VMEM(gate_ints.shape, jnp.int32),
            pltpu.SemaphoreType.DMA((3,)),
        ],
        compiler_params=LIMIT,
        name="head",
    )(me, *in_hbm(tokens, expert_ids, gate_ints))
    own = lax.all_to_all(tiled, ALL, split_axis=0, concat_axis=0, axis_index_groups=groups, tiled=True)
    own = own.reshape(n * tokens.shape[0], width + LANES)
    wg, wu, wd = pl.pallas_call(
        load_kernel,
        out_shape=[jax.ShapeDtypeStruct(w.shape[1:], bf16) for w in (w_gate, w_up, w_down)],
        in_specs=[HBM] * 3 + [pl.BlockSpec(memory_space=pl.ANY)],
        out_specs=[VMEM] * 3,
        scratch_shapes=[pltpu.SemaphoreType.DMA((3,))],
        compiler_params=LIMIT,
        cost_estimate=cost(3.4),
        name="load",
    )(*in_hbm(w_gate[0], w_up[0], w_down[0]), own)

    near = {a: moved(own, neighbour_pairs(a)) for a in "xyz"}
    near["o"] = own
    swapped = {a: moved(b, swap_pairs()) for a, b in near.items()}
    total = {}
    after = me
    for pair in ("xo", "yz"):
        mine, theirs = run_experts(me, [near[a] for a in pair], [swapped[a] for a in pair], (wg, wu, wd), after)
        after = theirs[0]
        for a, kept, sent in zip(pair, mine, theirs):
            total[a] = kept + moved(sent, swap_pairs()).astype(f32)
    acc = total["o"]
    for a in "xyz":
        acc = acc + moved(total[a].astype(bf16), neighbour_pairs(a)).astype(f32)
    pieces = acc.astype(bf16).reshape(n, tokens.shape[0], width)
    got = lax.all_to_all(pieces, ALL, split_axis=0, concat_axis=0, axis_index_groups=groups, tiled=True)
    return jnp.sum(got.astype(f32), axis=0).astype(bf16)


def solution(mesh):
    fine = Mesh(mesh.devices.reshape(RING, RING, RING, 2), ALL)
    in_specs = (
        P(ALL, None),
        P(ALL, None),
        P(ALL, None),
        P(("z", "x"), None, ("y", "c")),
        P(("z", "x"), None, ("y", "c")),
        P(("z", "x"), ("y", "c"), None),
    )
    return jax.shard_map(step, mesh=fine, in_specs=in_specs, out_specs=P(ALL, None), check_vma=False)
```

```python
import itertools

import jax
import jax.numpy as jnp
from jax import lax
from jax.experimental import pallas as pl
from jax.experimental.pallas import tpu as pltpu
from jax.sharding import Mesh
from jax.sharding import PartitionSpec as P

ALL = ("z", "x", "y", "c")
RING = 4
LANES = 128
KCH = 1024
RATE = 250


def index(z, x, y, c):
    return ((z * RING + x) * RING + y) * 2 + c


def apart(u, v):
    return sum(min((p - q) % RING, (q - p) % RING) for p, q in zip(u, v))


def class_groups():
    groups = []
    for a, b, c in itertools.product(range(2), repeat=3):
        left = []
        for z, x, y in itertools.product(range(RING), repeat=3):
            if (x + z) % 2 == a and (y + z) % 2 == b:
                left.append((z, x, y))
        first, second = [], []
        while left:
            chip = left.pop(0)
            first.append(chip)
            second.append(left.pop(max(range(len(left)), key=lambda i: apart(left[i], chip))))
        groups.append([index(z, x, y, c) for z, x, y in first + second])
    return groups


def neighbour_pairs(axis):
    pairs = []
    for z, x, y in itertools.product(range(RING), repeat=3):
        for c in range(2):
            there = {"z": z, "x": x, "y": y}
            there[axis] = RING - 1 - there[axis] if c else there[axis] ^ 1
            pairs.append((index(z, x, y, c), index(there["z"], there["x"], there["y"], c)))
    return pairs


def swap_pairs():
    return [(i, i ^ 1) for i in range(2 * RING**3)]


def head_kernel(me_ref, tok_hbm, ids_hbm, ints_hbm, out_ref, tok, ids_ref, ints_ref, sems):
    width = tok.shape[1]
    copies = [
        pltpu.make_async_copy(src, dst, sems.at[i])
        for i, (src, dst) in enumerate(((ids_hbm, ids_ref), (ints_hbm, ints_ref), (tok_hbm, tok)))
    ]
    for copy in copies:
        copy.start()
    for copy in copies:
        copy.wait()
    ids, ints = ids_ref[...], ints_ref[...]
    lane = lax.broadcasted_iota(jnp.int32, (ids.shape[0], LANES), 1)
    scores = jnp.zeros(lane.shape, jnp.float32)
    for k in range(ids.shape[1]):
        scores += jnp.where(ids[:, k:k + 1] == lane, ints[:, k:k + 1], 0).astype(jnp.float32)
    scores = scores.astype(jnp.bfloat16)
    token = tok[...]
    for i in range(out_ref.shape[0]):
        out_ref[i, :, :width] = token
        out_ref[i, :, width:] = scores


def sum_kernel(got_ref, out_ref):
    out_ref[...] = jnp.sum(got_ref[...].astype(jnp.float32), axis=0).astype(jnp.bfloat16)


def load_kernel(wg_hbm, wu_hbm, wd_hbm, after_ref, wg, wu, wd, sems):
    copies = [
        pltpu.make_async_copy(src, dst, sems.at[i])
        for i, (src, dst) in enumerate(((wg_hbm, wg), (wu_hbm, wu), (wd_hbm, wd)))
    ]
    for copy in copies:
        copy.start()
    for copy in copies:
        copy.wait()


def experts_kernel(me_ref, *refs):
    ins, (wg, wu, wd, after_ref), outs, hid = refs[:4], refs[4:8], refs[8:12], refs[12]
    width = wg.shape[0]
    size = ins[0].shape[0]

    def rows(ks):
        return jnp.concatenate([r[:, ks] for r in ins], axis=0)

    scores = rows(pl.ds(width, LANES)).astype(jnp.float32)
    lane = lax.broadcasted_iota(jnp.int32, scores.shape, 1)
    picked = jnp.sum(jnp.where(lane == me_ref[0], scores, 0.0), axis=1, keepdims=True)
    weight = picked / jnp.sum(scores, axis=1, keepdims=True)
    gate = up = None
    for i in range(width // KCH):
        ks = pl.ds(i * KCH, KCH)
        part = rows(ks)
        g = jnp.dot(part, wg[ks, :], preferred_element_type=jnp.float32)
        u = jnp.dot(part, wu[ks, :], preferred_element_type=jnp.float32)
        gate, up = (g, u) if gate is None else (gate + g, up + u)
    hid[...] = (gate / (1.0 + jnp.exp(-gate)) * up).astype(jnp.bfloat16)
    for i in range(width // KCH):
        ks = pl.ds(i * KCH, KCH)
        out = jnp.dot(hid[...], wd[:, ks], preferred_element_type=jnp.float32) * weight
        for j, ref in enumerate(outs):
            ref[:, ks] = out[j * size:(j + 1) * size].astype(ref.dtype)


def run_experts(me, mine, theirs, weights, after):
    size = mine[0].shape[0]
    width, hidden = weights[0].shape
    kinds = [jnp.float32] * 2 + [jnp.bfloat16] * 2
    outs = pl.pallas_call(
        experts_kernel,
        out_shape=[jax.ShapeDtypeStruct((size, width), kind) for kind in kinds],
        in_specs=[SMEM] + [VMEM] * 7 + [pl.BlockSpec(memory_space=pl.ANY)],
        out_specs=[VMEM] * 4,
        scratch_shapes=[pltpu.VMEM((4 * size, hidden), jnp.bfloat16)],
        compiler_params=LIMIT,
        cost_estimate=cost(1.8),
    )(me, *mine, *theirs, *weights, after)
    return outs[:2], outs[2:]


VMEM = pl.BlockSpec(memory_space=pltpu.VMEM)
SMEM = pl.BlockSpec(memory_space=pltpu.SMEM)
HBM = pl.BlockSpec(memory_space=pltpu.HBM)
LIMIT = pltpu.CompilerParams(vmem_limit_bytes=24 * 1024 * 1024)


def cost(us):
    return pl.CostEstimate(flops=int(us * 1e6 * RATE), transcendentals=0, bytes_accessed=0)


def in_hbm(*arrays):
    return [pltpu.with_memory_space_constraint(a, pltpu.HBM) for a in arrays]


def moved(block, pairs):
    return lax.ppermute(block, ALL, pairs)


def step(tokens, expert_ids, gate_ints, w_gate, w_up, w_down):
    width = tokens.shape[1]
    me = (lax.axis_index("z") * RING + lax.axis_index("x")).astype(jnp.int32).reshape(1)
    groups = class_groups()
    n = len(groups[0])
    bf16, f32 = jnp.bfloat16, jnp.float32

    tiled = pl.pallas_call(
        head_kernel,
        out_shape=jax.ShapeDtypeStruct((n, tokens.shape[0], width + LANES), bf16),
        in_specs=[SMEM] + [HBM] * 3,
        out_specs=VMEM,
        scratch_shapes=[
            pltpu.VMEM(tokens.shape, bf16),
            pltpu.VMEM(expert_ids.shape, jnp.int32),
            pltpu.VMEM(gate_ints.shape, jnp.int32),
            pltpu.SemaphoreType.DMA((3,)),
        ],
        compiler_params=LIMIT,
        name="head",
    )(me, *in_hbm(tokens, expert_ids, gate_ints))
    own = lax.all_to_all(tiled, ALL, split_axis=0, concat_axis=0, axis_index_groups=groups, tiled=True)
    own = own.reshape(n * tokens.shape[0], width + LANES)
    wg, wu, wd = pl.pallas_call(
        load_kernel,
        out_shape=[jax.ShapeDtypeStruct(w.shape[1:], bf16) for w in (w_gate, w_up, w_down)],
        in_specs=[HBM] * 3 + [pl.BlockSpec(memory_space=pl.ANY)],
        out_specs=[VMEM] * 3,
        scratch_shapes=[pltpu.SemaphoreType.DMA((3,))],
        compiler_params=LIMIT,
        cost_estimate=cost(3.4),
        name="load",
    )(*in_hbm(w_gate[0], w_up[0], w_down[0]), own)

    near = {a: moved(own, neighbour_pairs(a)) for a in "xyz"}
    near["o"] = own
    swapped = {a: moved(b, swap_pairs()) for a, b in near.items()}
    total = {}
    after = me
    for pair in ("xo", "yz"):
        mine, theirs = run_experts(me, [near[a] for a in pair], [swapped[a] for a in pair], (wg, wu, wd), after)
        after = theirs[0]
        for a, kept, sent in zip(pair, mine, theirs):
            total[a] = kept + moved(sent, swap_pairs()).astype(f32)
    acc = total["o"]
    for a in "xyz":
        acc = acc + moved(total[a].astype(bf16), neighbour_pairs(a)).astype(f32)
    pieces = acc.astype(bf16).reshape(n, tokens.shape[0], width)
    got = lax.all_to_all(pieces, ALL, split_axis=0, concat_axis=0, axis_index_groups=groups, tiled=True)
    lanes = width // LANES
    pairs = tokens.shape[0] * lanes
    got = got.reshape(n, tokens.shape[0], lanes, LANES).transpose(0, 2, 1, 3).reshape(n, pairs, LANES)
    out = pl.pallas_call(
        sum_kernel,
        out_shape=jax.ShapeDtypeStruct((pairs, LANES), bf16),
        in_specs=[VMEM],
        out_specs=VMEM,
        compiler_params=LIMIT,
        name="sum",
    )(got)
    return out.reshape(lanes, tokens.shape[0], LANES).transpose(1, 0, 2).reshape(tokens.shape)


def solution(mesh):
    fine = Mesh(mesh.devices.reshape(RING, RING, RING, 2), ALL)
    in_specs = (
        P(ALL, None),
        P(ALL, None),
        P(ALL, None),
        P(("z", "x"), None, ("y", "c")),
        P(("z", "x"), None, ("y", "c")),
        P(("z", "x"), ("y", "c"), None),
    )
    return jax.shard_map(step, mesh=fine, in_specs=in_specs, out_specs=P(ALL, None), check_vma=False)
```

```python
import itertools

import jax
import jax.numpy as jnp
from jax import lax
from jax.experimental import pallas as pl
from jax.experimental.pallas import tpu as pltpu
from jax.sharding import Mesh
from jax.sharding import PartitionSpec as P

ALL = ("z", "x", "y", "c")
RING = 4
LANES = 128
KCH = 1024
DOWN = 3584
RATE = 250


def index(z, x, y, c):
    return ((z * RING + x) * RING + y) * 2 + c


def apart(u, v):
    return sum(min((p - q) % RING, (q - p) % RING) for p, q in zip(u, v))


def class_groups():
    groups = []
    for a, b, c in itertools.product(range(2), repeat=3):
        left = []
        for z, x, y in itertools.product(range(RING), repeat=3):
            if (x + z) % 2 == a and (y + z) % 2 == b:
                left.append((z, x, y))
        first, second = [], []
        while left:
            chip = left.pop(0)
            first.append(chip)
            second.append(left.pop(max(range(len(left)), key=lambda i: apart(left[i], chip))))
        groups.append([index(z, x, y, c) for z, x, y in first + second])
    return groups


def neighbour_pairs(axis):
    pairs = []
    for z, x, y in itertools.product(range(RING), repeat=3):
        for c in range(2):
            there = {"z": z, "x": x, "y": y}
            there[axis] = RING - 1 - there[axis] if c else there[axis] ^ 1
            pairs.append((index(z, x, y, c), index(there["z"], there["x"], there["y"], c)))
    return pairs


def swap_pairs():
    return [(i, i ^ 1) for i in range(2 * RING**3)]


def head_kernel(me_ref, tok_hbm, ids_hbm, ints_hbm, out_ref, tok, ids_ref, ints_ref, sems):
    width = tok.shape[1]
    copies = [
        pltpu.make_async_copy(src, dst, sems.at[i])
        for i, (src, dst) in enumerate(((ids_hbm, ids_ref), (ints_hbm, ints_ref), (tok_hbm, tok)))
    ]
    for copy in copies:
        copy.start()
    for copy in copies:
        copy.wait()
    ids, ints = ids_ref[...], ints_ref[...]
    lane = lax.broadcasted_iota(jnp.int32, (ids.shape[0], LANES), 1)
    scores = jnp.zeros(lane.shape, jnp.float32)
    for k in range(ids.shape[1]):
        scores += jnp.where(ids[:, k:k + 1] == lane, ints[:, k:k + 1], 0).astype(jnp.float32)
    scores = scores.astype(jnp.bfloat16)
    token = tok[...]
    for i in range(out_ref.shape[0]):
        out_ref[i, :, :width] = token
        out_ref[i, :, width:] = scores


def sum_kernel(got_ref, out_ref):
    out_ref[...] = jnp.sum(got_ref[...].astype(jnp.float32), axis=0).astype(jnp.bfloat16)


def add_kernel(kept, b0, b1, b2, b3, out_ref):
    rows = out_ref.shape[1]
    for i in range(kept.shape[1] // KCH):
        ks = pl.ds(i * KCH, KCH)
        acc = kept[:, ks]
        for ref in (b0, b1, b2, b3):
            acc = acc + ref[:, ks].astype(jnp.float32)
        acc = acc.astype(jnp.bfloat16)
        for j in range(out_ref.shape[0]):
            out_ref[j, :, ks] = acc[j * rows:(j + 1) * rows]


def load_kernel(wg_hbm, wu_hbm, wd_hbm, after_ref, wg, wu, wd, sems):
    copies = [
        pltpu.make_async_copy(src, dst, sems.at[i])
        for i, (src, dst) in enumerate(((wg_hbm, wg), (wu_hbm, wu), (wd_hbm, wd)))
    ]
    for copy in copies:
        copy.start()
    for copy in copies:
        copy.wait()


def experts_kernel(me_ref, *refs):
    ins, (wg, wu, wd, after_ref), outs, hid = refs[:4], refs[4:8], refs[8:12], refs[12]
    width = wg.shape[0]
    size = ins[0].shape[0]

    def rows(ks):
        return jnp.concatenate([r[:, ks] for r in ins], axis=0)

    scores = rows(pl.ds(width, LANES)).astype(jnp.float32)
    lane = lax.broadcasted_iota(jnp.int32, scores.shape, 1)
    picked = jnp.sum(jnp.where(lane == me_ref[0], scores, 0.0), axis=1, keepdims=True)
    weight = picked / jnp.sum(scores, axis=1, keepdims=True)
    gate = up = None
    for i in range(width // KCH):
        ks = pl.ds(i * KCH, KCH)
        part = rows(ks)
        g = jnp.dot(part, wg[ks, :], preferred_element_type=jnp.float32)
        u = jnp.dot(part, wu[ks, :], preferred_element_type=jnp.float32)
        gate, up = (g, u) if gate is None else (gate + g, up + u)
    hid[...] = (gate / (1.0 + jnp.exp(-gate)) * up).astype(jnp.bfloat16)
    for i in range(width // DOWN):
        ks = pl.ds(i * DOWN, DOWN)
        out = jnp.dot(hid[...], wd[:, ks], preferred_element_type=jnp.float32) * weight
        for j, ref in enumerate(outs):
            ref[:, ks] = out[j * size:(j + 1) * size].astype(ref.dtype)


def run_experts(me, mine, theirs, weights, after):
    size = mine[0].shape[0]
    width, hidden = weights[0].shape
    kinds = [jnp.float32] * 2 + [jnp.bfloat16] * 2
    outs = pl.pallas_call(
        experts_kernel,
        out_shape=[jax.ShapeDtypeStruct((size, width), kind) for kind in kinds],
        in_specs=[SMEM] + [VMEM] * 7 + [pl.BlockSpec(memory_space=pl.ANY)],
        out_specs=[VMEM] * 4,
        scratch_shapes=[pltpu.VMEM((4 * size, hidden), jnp.bfloat16)],
        compiler_params=LIMIT,
        cost_estimate=cost(1.8),
    )(me, *mine, *theirs, *weights, after)
    return outs[:2], outs[2:]


VMEM = pl.BlockSpec(memory_space=pltpu.VMEM)
SMEM = pl.BlockSpec(memory_space=pltpu.SMEM)
HBM = pl.BlockSpec(memory_space=pltpu.HBM)
LIMIT = pltpu.CompilerParams(vmem_limit_bytes=24 * 1024 * 1024)


def cost(us):
    return pl.CostEstimate(flops=int(us * 1e6 * RATE), transcendentals=0, bytes_accessed=0)


def in_hbm(*arrays):
    return [pltpu.with_memory_space_constraint(a, pltpu.HBM) for a in arrays]


def moved(block, pairs):
    return lax.ppermute(block, ALL, pairs)


def step(tokens, expert_ids, gate_ints, w_gate, w_up, w_down):
    width = tokens.shape[1]
    me = (lax.axis_index("z") * RING + lax.axis_index("x")).astype(jnp.int32).reshape(1)
    groups = class_groups()
    n = len(groups[0])
    bf16, f32 = jnp.bfloat16, jnp.float32

    tiled = pl.pallas_call(
        head_kernel,
        out_shape=jax.ShapeDtypeStruct((n, tokens.shape[0], width + LANES), bf16),
        in_specs=[SMEM] + [HBM] * 3,
        out_specs=VMEM,
        scratch_shapes=[
            pltpu.VMEM(tokens.shape, bf16),
            pltpu.VMEM(expert_ids.shape, jnp.int32),
            pltpu.VMEM(gate_ints.shape, jnp.int32),
            pltpu.SemaphoreType.DMA((3,)),
        ],
        compiler_params=LIMIT,
        name="head",
    )(me, *in_hbm(tokens, expert_ids, gate_ints))
    own = lax.all_to_all(tiled, ALL, split_axis=0, concat_axis=0, axis_index_groups=groups, tiled=True)
    own = own.reshape(n * tokens.shape[0], width + LANES)
    wg, wu, wd = pl.pallas_call(
        load_kernel,
        out_shape=[jax.ShapeDtypeStruct(w.shape[1:], bf16) for w in (w_gate, w_up, w_down)],
        in_specs=[HBM] * 3 + [pl.BlockSpec(memory_space=pl.ANY)],
        out_specs=[VMEM] * 3,
        scratch_shapes=[pltpu.SemaphoreType.DMA((3,))],
        compiler_params=LIMIT,
        cost_estimate=cost(3.4),
        name="load",
    )(*in_hbm(w_gate[0], w_up[0], w_down[0]), own)

    near = {a: moved(own, neighbour_pairs(a)) for a in "yzx"}
    near["o"] = own
    swapped = {a: moved(b, swap_pairs()) for a, b in near.items()}
    total, parts = {}, {}
    after = me
    for pair in ("yo", "zx"):
        mine, theirs = run_experts(me, [near[a] for a in pair], [swapped[a] for a in pair], (wg, wu, wd), after)
        after = theirs[0]
        for a, kept, sent in zip(pair, mine, theirs):
            parts[a] = (kept, moved(sent, swap_pairs()))
            total[a] = parts[a][0] + parts[a][1].astype(f32)
    arrived = [moved(total[a].astype(bf16), neighbour_pairs(a)) for a in "yzx"]
    pieces = pl.pallas_call(
        add_kernel,
        out_shape=jax.ShapeDtypeStruct((n, tokens.shape[0], width), bf16),
        in_specs=[VMEM] * 5,
        out_specs=VMEM,
        compiler_params=LIMIT,
        name="add",
    )(*parts["o"], *arrived)
    got = lax.all_to_all(pieces, ALL, split_axis=0, concat_axis=0, axis_index_groups=groups, tiled=True)
    lanes = width // LANES
    pairs = tokens.shape[0] * lanes
    got = got.reshape(n, tokens.shape[0], lanes, LANES).transpose(0, 2, 1, 3).reshape(n, pairs, LANES)
    out = pl.pallas_call(
        sum_kernel,
        out_shape=jax.ShapeDtypeStruct((pairs, LANES), bf16),
        in_specs=[VMEM],
        out_specs=VMEM,
        compiler_params=LIMIT,
        name="sum",
    )(got)
    return out.reshape(lanes, tokens.shape[0], LANES).transpose(1, 0, 2).reshape(tokens.shape)


def solution(mesh):
    fine = Mesh(mesh.devices.reshape(RING, RING, RING, 2), ALL)
    in_specs = (
        P(ALL, None),
        P(ALL, None),
        P(ALL, None),
        P(("z", "x"), None, ("y", "c")),
        P(("z", "x"), None, ("y", "c")),
        P(("z", "x"), ("y", "c"), None),
    )
    return jax.shard_map(step, mesh=fine, in_specs=in_specs, out_specs=P(ALL, None), check_vma=False)
```
